32 devices in a mesh: dom: 8 (over z, x), feat: 4 (over y, core).
Axes of the slice: x: 2, y: 2, z: 4, core: 2. Of those that a mesh axis runs over, the one named last changes fastest.
Arguments:
- feats: bfloat16 [256, 4096], P('feat', 'dom'), may hold values from -6 to 6
- self_weight: bfloat16 [256, 256], P(None, 'feat'), may hold values from -0.375 to 0.375
- bases: bfloat16 [30, 256, 256], P(None, 'feat'), may hold values from -0.375 to 0.375
- coef: float32 [237, 30], replicated, may hold values from -1.2 to 1.2
- src_part: int32 [8192, 1], P('dom'), may hold values from 0 to 7; in each aligned block of 1024 rows (0 to 1023, 1024 to 2047, ...) at most 256 rows name the same one
- src_row: int32 [8192], P('dom'), may hold values from 0 to 511
- edge_dst: int32 [8192], P('dom'), may hold values from 0 to 511
- edge_rel: int32 [8192], P('dom'), may hold values from 0 to 236
- block_owner: int32 [64, 1], P('dom'), may hold values from 0 to 7; in each aligned block of 8 rows (0 to 7, 8 to 15, ...) at most 2 rows name the same one
- block_valid: int32 [8, 8], P('dom'), may hold values from 1 to 128, 896 in all within a row
- cotangent: bfloat16 [256, 4096], P('feat', 'dom'), may hold values from -6 to 6
Outputs:
- output: bfloat16 [256, 4096], P('feat', 'dom')
- grad_feats: bfloat16 [256, 4096], P('feat', 'dom')
- grad_bases: float32 [30, 256, 256], P(None, 'feat')
- grad_self: float32 [256, 256], P(None, 'feat')
- grad_coef: float32 [237, 30], replicated
The draws below stay inside these ranges and needn't reach their ends.
Inputs may be any that keep to these rules, and one draw needn't show every extreme that they name: `src_part`: among the edge rows of one index of dom, no partition is the source partition of more than 256 rows, and some partition of exactly 256. `block_owner`: among the blocks of one index of dom, no partition owns more than 2, a bound that some block reaches. `block_valid`: the valid rows of a block come first; the counts of one index of dom sum to 896.
All inputs are finite; a program needn't handle non-finite values.
Results may differ from the reference program's by a relative error of at most 0.0055.
Values may be sent and summed in bfloat16 or wider, within the bound.
A program may use at most 64 MiB of HBM per device.

```python
import math
import jax
import jax.numpy as jnp
import numpy as np
from jax import lax

D = 256
BASES = 30
RELS = 237
ROWS = 128
ENT_DEV = 512
NB = 8
EDGE_DEV = 1024
ENTITIES = 4096
EDGES = 8192
BLOCKS = 64
SCAP = 256
BCAP = 2
VALID_DEV = 896
N_DOM = 8


def set_ends(result, own_key, smallest, top_value):
    longest = result.shape.index(max(result.shape))
    spots = []
    for shift in (0, 1):
        where = [jax.random.randint(jax.random.fold_in(own_key, axis), (), 0, length) for axis, length in enumerate(result.shape)]
        where[longest] = (where[longest] + shift) % result.shape[longest]
        spots.append(tuple(where))
    return result.at[spots[0]].set(smallest).at[spots[1]].set(top_value)


def shard_levels(own_key, extent, pieces, least, high):
    factor_of = 1.0
    for position, shards_of in pieces:
        steps = jax.random.uniform(jax.random.fold_in(jax.random.fold_in(own_key, 6), position), (shards_of,), jnp.float32, least / len(pieces), high / len(pieces))
        factor_of = factor_of * jnp.repeat(jnp.exp(steps), extent[position] // shards_of).reshape((-1,) + (1,) * (len(extent) - 1 - position))
    return factor_of


def rank_bounds(amount, lean):
    loads = [(1 << 20) // math.isqrt(rank ** lean) + 1 for rank in range(1, amount + 1)]
    scale = 1 + sum(loads) // (1 << 30)
    return np.cumsum(np.array([max(1, weight // scale) for weight in loads]))


def skewed_ids(rng, extent, number_of, skew):
    grid = rank_bounds(number_of, skew)
    lot = jax.random.randint(jax.random.fold_in(rng, 1), extent, 0, int(grid[number_of - 1]))
    grade = jnp.searchsorted(jnp.asarray(grid, jnp.int32), lot, side="right")
    return jax.random.permutation(jax.random.fold_in(rng, 2), number_of)[grade].astype(jnp.int32)


def length_profile(amount, total, most, skew):
    loads = [(1 << 20) // math.isqrt(grade ** skew) + 1 for grade in range(2, amount + 1)]
    rest, given = total - most - (amount - 1), [1] * (amount - 1)
    while rest > 0:
        movable = [i for i in range(amount - 1) if given[i] < most]
        whole, remaining = sum([loads[i] for i in movable]), rest
        for i in movable:
            addition = min(most - given[i], max(1, remaining * loads[i] // whole), rest)
            given[i] = given[i] + addition
            rest = rest - addition
    return np.array([most] + given)


def uneven_parts(own_key, count, total, bound, slope):
    if count == 2:
        one = jax.random.randint(own_key, (), max(1, total - bound), min(bound, total - 1) + 1)
        return jnp.stack([one, total - one])
    sizes = jnp.asarray(length_profile(count, total, bound, slope), jnp.int32)
    couples = (count - 1) // 2
    source_of, sink = sizes[1:1 + 2 * couples:2], sizes[2:2 + 2 * couples:2]
    margin = jnp.minimum(source_of - 1, bound - sink)
    shifted = jax.random.randint(jax.random.fold_in(own_key, 1), (couples,), 0, 1 << 20) % (margin + 1)
    sizes = sizes.at[1:1 + 2 * couples:2].set(source_of - shifted).at[2:2 + 2 * couples:2].set(sink + shifted)
    return sizes[jax.random.permutation(jax.random.fold_in(own_key, 2), count)]


def deal_out(own_key, own, number, rows, number_of, top, limit, slope):
    order = jax.random.permutation(own_key, number_of)
    packed, ordinary = load_shares(number_of, rows * top, limit, slope, True), load_shares(number_of, rows * top, limit, slope, False)
    places = jnp.arange(number_of)

    def named(tallies, rotation):
        used = int((tallies > 0).sum())
        fixed = max(1, used // 4)
        moved = fixed + (places - fixed + rotation * (used - fixed)) % max(1, number_of - fixed)
        return jnp.zeros((number_of,), jnp.int32).at[order[jnp.where(places < fixed, places, moved)]].set(jnp.asarray(tallies, jnp.int32))

    tallies = jnp.where(number % 4 == 0, named(packed, number // 4), named(ordinary, number - number // 4 - 1))
    mixed = jax.random.permutation(jax.random.fold_in(own, 3), number_of)
    giver, receiver = mixed[0:number_of // 2 * 2:2], mixed[1:number_of // 2 * 2:2]
    room = jnp.minimum(tallies[giver] - 1, limit - tallies[receiver]) // 2
    room = jnp.where((giver == order[0]) | (receiver == order[0]) | (tallies[receiver] == 0), 0, jnp.maximum(room, 0))
    moved = jax.random.randint(jax.random.fold_in(own, 4), (number_of // 2,), 0, 1 << 20) % (room + 1)
    tallies = tallies.at[giver].add(-moved).at[receiver].add(moved)
    labels = jnp.searchsorted(jnp.cumsum(tallies), jnp.arange(rows * top), side="right").astype(jnp.int32)
    grid = labels.reshape(top, rows).T
    grid = grid[jax.random.permutation(jax.random.fold_in(own, 1), rows)]
    rotation = jax.random.randint(jax.random.fold_in(own, 2), (rows, 1), 0, top)
    return jnp.take_along_axis(grid, (jnp.arange(top)[None, :] + rotation) % top, axis=1)


def load_shares(count, total, bound, skew, full):
    loads = [(1 << 20) // math.isqrt(standing ** skew) + 1 for standing in range(1, count + 1)]
    largest = bound if full else min(bound, max(-(-total // count), total * loads[0] // sum(loads)))
    least = 1 if total - largest >= count - 1 else 0
    given, rest = [largest] + [least] * (count - 1), total - largest - least * (count - 1)
    while rest > 0:
        free = [i for i in range(1, count) if given[i] < largest] or [i for i in range(1, count) if given[i] < bound]
        mass, remaining = sum([loads[i] for i in free]), rest
        for i in free:
            extra = min(bound - given[i], max(1, remaining * loads[i] // mass), rest)
            given[i] = given[i] + extra
            rest = rest - extra
    return np.array(given)


def normal_values(stream_key, extent, width, bound, pieces=(), held_as=jnp.bfloat16):
    array = jax.random.normal(stream_key, extent, jnp.float32) * width
    if len(pieces) > 0:
        array = shard_levels(stream_key, extent, pieces, -0.22, 0.18) * array
    return jnp.clip(array, min=-bound, max=bound).astype(held_as)


def setup_inputs(seed: int = 0) -> dict:
    key_list = jax.random.split(jax.random.key(seed), 12)
    feats = normal_values(key_list[0], (D, ENTITIES), 1.0, 6.0, ((0, 4), (1, 8)))
    self_weight = normal_values(key_list[1], (D, D), D ** -0.5, 0.375, ((1, 4),))
    bases = normal_values(key_list[2], (BASES, D, D), D ** -0.5, 0.375, ((1, 4),))
    coef = normal_values(key_list[3], (RELS, BASES), 0.2, 1.2, (), jnp.float32)
    src_part_keys = jax.random.split(jax.random.fold_in(key_list[4], 1), EDGES // EDGE_DEV)
    src_part_turns = jax.random.permutation(jax.random.fold_in(key_list[4], 3), EDGES // EDGE_DEV)
    src_part = jax.vmap(lambda own, number: deal_out(jax.random.fold_in(key_list[4], 2), own, number, EDGE_DEV, N_DOM, 1, SCAP, 2))(src_part_keys, src_part_turns).reshape((EDGES, 1))
    src_row = set_ends(jax.random.randint(key_list[5], (EDGES,), 0, ENT_DEV), jax.random.fold_in(key_list[5], 1), 0, ENT_DEV - 1).astype(jnp.int32)
    edge_dst = set_ends(jax.random.randint(key_list[6], (EDGES,), 0, ENT_DEV), jax.random.fold_in(key_list[6], 1), 0, ENT_DEV - 1).astype(jnp.int32)
    edge_rel = set_ends(skewed_ids(key_list[7], (EDGES,), RELS, 2), jax.random.fold_in(key_list[7], 3), 0, RELS - 1).astype(jnp.int32)
    block_owner_keys = jax.random.split(jax.random.fold_in(key_list[8], 1), BLOCKS // NB)
    block_owner_turns = jax.random.permutation(jax.random.fold_in(key_list[8], 3), BLOCKS // NB)
    block_owner = jax.vmap(lambda own, number: deal_out(jax.random.fold_in(key_list[8], 2), own, number, NB, N_DOM, 1, BCAP, 2))(block_owner_keys, block_owner_turns).reshape((BLOCKS, 1))
    block_valid = jax.vmap(lambda own: uneven_parts(own, NB, VALID_DEV, ROWS, 2))(jax.random.split(key_list[9], N_DOM)).reshape((N_DOM, NB)).astype(jnp.int32)
    cotangent = normal_values(key_list[10], (D, ENTITIES), 1.0, 6.0, ((0, 4), (1, 8)))
    return dict(feats=feats, self_weight=self_weight, bases=bases, coef=coef, src_part=src_part, src_row=src_row, edge_dst=edge_dst, edge_rel=edge_rel, block_owner=block_owner, block_valid=block_valid, cotangent=cotangent)


def float_dot(left, right):
    return jnp.dot(left.astype(jnp.float32), right.astype(jnp.float32), precision=lax.Precision.HIGHEST)


def reference(feats, self_weight, bases, coef, src_part, src_row, edge_dst, edge_rel, block_owner, block_valid, cotangent):
    entity_total = ENT_DEV * N_DOM
    edge_total = EDGE_DEV * N_DOM
    source_ids = (src_part[:, 0] * ENT_DEV + src_row).astype(jnp.int32)
    owners = jnp.repeat(block_owner[:, 0], ROWS)
    live_rows = (jnp.arange(ROWS, dtype=jnp.int32)[None, :] < block_valid.reshape(-1)[:, None]).reshape(-1)
    target_ids = (owners * ENT_DEV + edge_dst).astype(jnp.int32)
    live_float = live_rows.astype(jnp.float32)
    degree = jnp.zeros((entity_total,), jnp.float32).at[target_ids].add(live_float)
    inverse_degree = 1.0 / jnp.maximum(degree, 1.0)
    edge_coef = coef[edge_rel]
    bases_flat = jnp.transpose(bases, (2, 0, 1)).reshape(D, BASES * D).astype(jnp.float32)
    grouped = (source_ids.reshape(N_DOM, EDGE_DEV), target_ids.reshape(N_DOM, EDGE_DEV),
               edge_coef.reshape(N_DOM, EDGE_DEV, BASES), live_float.reshape(N_DOM, EDGE_DEV),
               edge_rel.reshape(N_DOM, EDGE_DEV))

    def basis_products(src_ids):
        source_feats = feats[:, src_ids].astype(jnp.float32)
        products = jnp.dot(source_feats.T, bases_flat, precision=lax.Precision.HIGHEST)
        return source_feats, products.reshape(-1, BASES, D)

    def forward_group(aggregate, group):
        src_ids, dst_ids, weights, live, rels = group
        source_feats, products = basis_products(src_ids)
        message = jnp.einsum("eb,ebo->eo", weights, products, precision=lax.Precision.HIGHEST)
        message = (message * live[:, None]).astype(jnp.bfloat16)
        return aggregate.at[dst_ids].add(message.astype(jnp.float32)), jnp.zeros((), jnp.float32)

    aggregate, ignored = lax.scan(forward_group, jnp.zeros((entity_total, D), jnp.float32), grouped)
    preact = float_dot(feats.T, self_weight) + inverse_degree[:, None] * aggregate
    output = jax.nn.silu(preact).astype(jnp.bfloat16)
    sigmoid_pre = jax.nn.sigmoid(preact)
    grad_pre = (cotangent.T.astype(jnp.float32) * sigmoid_pre * (1.0 + preact * (1.0 - sigmoid_pre))).astype(jnp.bfloat16)

    def backward_group(totals_now, group):
        grad_bases, grad_coef, edge_grads = totals_now
        src_ids, dst_ids, weights, live, rels = group
        source_feats, products = basis_products(src_ids)
        grad_message = inverse_degree[dst_ids][:, None] * grad_pre[dst_ids].astype(jnp.float32) * live[:, None]
        grad_message = grad_message.astype(jnp.bfloat16).astype(jnp.float32)
        scaled = jnp.einsum("ebo,eo->eb", products, grad_message, precision=lax.Precision.HIGHEST)
        grad_coef = grad_coef + jax.ops.segment_sum(scaled, rels, num_segments=RELS)
        combined = (weights[:, :, None] * grad_message[:, None, :]).astype(jnp.bfloat16).reshape(-1, BASES * D)
        grad_bases = grad_bases + float_dot(source_feats, combined)
        edge_part = float_dot(combined, bases_flat.T)
        edge_grads = edge_grads.at[src_ids].add(edge_part)
        return (grad_bases, grad_coef, edge_grads), jnp.zeros((), jnp.float32)

    start_state = (jnp.zeros((D, BASES * D), jnp.float32), jnp.zeros((RELS, BASES), jnp.float32),
                   jnp.zeros((entity_total, D), jnp.float32))
    final_state, ignored = lax.scan(backward_group, start_state, grouped)
    grad_bases, grad_coef, edge_grads = final_state
    self_part = float_dot(grad_pre, self_weight.T)
    grad_feats = (self_part + edge_grads).astype(jnp.bfloat16).T
    grad_self = float_dot(feats, grad_pre)
    scale = float(edge_total) ** -0.5
    grad_bases = jnp.transpose((grad_bases * scale).reshape(D, BASES, D), (1, 2, 0))
    return (output.T, grad_feats, grad_bases, grad_self * scale, grad_coef * scale)
```

```python
import jax
import jax.numpy as jnp
from jax import lax
from jax.sharding import PartitionSpec as P

BF = jnp.bfloat16
F32 = jnp.float32


def dot(left, right, left_axis, right_axis):
    return lax.dot_general(
        left, right, (((left_axis,), (right_axis,)), ((), ())), preferred_element_type=F32
    )


def onehot(ids, start, size):
    return (jnp.arange(size, dtype=jnp.int32)[:, None] + start == ids[None, :]).astype(BF)


def pick(table, ids, chunk):
    width = table.shape[1]
    if width <= chunk:
        return dot(table, onehot(ids, 0, width), 1, 0).astype(BF)

    def step(index, total):
        piece = lax.dynamic_slice_in_dim(table, index * chunk, chunk, 1)
        return total + dot(piece, onehot(ids, index * chunk, chunk), 1, 0)

    total = lax.fori_loop(
        0, width // chunk, step, jnp.zeros((table.shape[0], ids.shape[0]), F32)
    )
    return total.astype(BF)


def spread(values, ids, width, chunk):
    if width <= chunk:
        return dot(values, onehot(ids, 0, width), 1, 1)

    def step(index, total):
        piece = dot(values, onehot(ids, index * chunk, chunk), 1, 1)
        return lax.dynamic_update_slice_in_dim(total, piece, index * chunk, 1)

    return lax.fori_loop(0, width // chunk, step, jnp.zeros((values.shape[0], width), F32))


def scatter_sum(values, axis, count):
    rows = values.shape[0]
    parts = lax.all_to_all(values, axis, split_axis=1, concat_axis=0, tiled=True)
    return jnp.sum(parts.reshape(count, rows, -1).astype(F32), axis=0)


def body(
    feats,
    self_weight,
    bases,
    coef,
    src_part,
    src_row,
    edge_dst,
    edge_rel,
    block_owner,
    block_valid,
    cotangent,
):
    dom_count = lax.axis_size("dom")
    feat_count = lax.axis_size("feat")
    quarter, entities = feats.shape
    edge_count = src_row.shape[0]
    block_count = block_valid.shape[1]
    block_rows = edge_count // block_count
    basis_count, _, width = bases.shape
    relations = coef.shape[0]
    total_entities = dom_count * entities
    chunk = min(8, dom_count) * entities
    scale = float(edge_count * dom_count) ** (-0.5)

    source_ids = src_part[:, 0] * entities + src_row
    live = (jnp.arange(block_rows)[None, :] < block_valid[0][:, None]).reshape(edge_count)
    owners = jnp.broadcast_to(block_owner, (block_count, block_rows)).reshape(edge_count)
    target_ids = jnp.where(live, owners * entities + edge_dst, -1)
    relation_hot = onehot(edge_rel, 0, relations)

    table = lax.all_gather(feats, "dom", axis=1, tiled=True)
    source_quarter = pick(table, source_ids, chunk)
    gathered = lax.all_gather(
        jnp.concatenate([source_quarter, feats], axis=1), "feat", axis=0, tiled=True
    )
    sources = gathered[:, :edge_count]
    own_full = gathered[:, edge_count:]

    bases_flat = bases.reshape(basis_count * quarter, width)
    first = coef.astype(BF)
    second = (coef - first.astype(F32)).astype(BF)
    third = (coef - first.astype(F32) - second.astype(F32)).astype(BF)
    weights = (
        dot(first, relation_hot, 0, 0)
        + dot(second, relation_hot, 0, 0)
        + dot(third, relation_hot, 0, 0)
    )
    products = dot(bases_flat, sources, 1, 0).reshape(basis_count, quarter, edge_count)
    messages = jnp.sum(weights[:, None, :] * products, axis=0).astype(BF)
    extra = 16
    tail = jnp.zeros((extra, edge_count), BF).at[0].set(1.0)
    partial = spread(jnp.concatenate([messages, tail], axis=0), target_ids, total_entities, chunk)
    counted = partial[quarter:quarter + 1]
    high = jnp.floor(counted / 128.0)
    counts = jnp.concatenate(
        [high, counted - 128.0 * high, jnp.zeros((extra - 2, total_entities), F32)], axis=0
    )
    arrived = scatter_sum(
        jnp.concatenate([partial[:quarter], counts], axis=0).astype(BF), "dom", dom_count
    )
    aggregate = arrived[:quarter]
    degree = arrived[quarter:quarter + 1] * 128.0 + arrived[quarter + 1:quarter + 2]
    inverse_degree = 1.0 / jnp.maximum(degree, 1.0)
    preact = dot(self_weight, own_full, 0, 0) + inverse_degree * aggregate
    output = jax.nn.silu(preact).astype(BF)
    sigmoid_pre = jax.nn.sigmoid(preact)
    grad_pre = (
        cotangent.astype(F32) * sigmoid_pre * (1.0 + preact * (1.0 - sigmoid_pre))
    ).astype(BF)
    grad_node = (grad_pre.astype(F32) * inverse_degree).astype(BF)
    grad_table = lax.all_gather(grad_node, "dom", axis=1, tiled=True)
    grad_message = pick(grad_table, target_ids, chunk)

    grad_float = grad_message.astype(F32)
    scaled = jnp.sum(products * grad_float[None], axis=1)
    combined = (weights[:, None, :] * grad_float[None]).astype(BF)
    combined = combined.reshape(basis_count * quarter, edge_count)
    grad_bases = dot(combined, sources, 1, 1)
    edge_partial = dot(bases_flat, combined, 0, 0)
    self_partial = dot(self_weight, grad_pre, 1, 0)
    self_term = dot(grad_pre, own_full, 1, 1)
    both = jnp.concatenate([edge_partial, self_partial], axis=1).astype(BF)
    both = lax.all_to_all(both, "feat", split_axis=0, concat_axis=0, tiled=True)
    both = jnp.sum(both.reshape(feat_count, quarter, -1).astype(F32), axis=0)
    edge_grads = both[:, :edge_count].astype(BF)
    self_grads = both[:, edge_count:]
    node_grads = spread(edge_grads, source_ids, total_entities, chunk).astype(BF)
    grad_feats = (self_grads + scatter_sum(node_grads, "dom", dom_count)).astype(BF)

    stacked = jnp.concatenate([grad_bases, self_term], axis=0).astype(BF)
    pieces = lax.all_to_all(stacked, "dom", split_axis=0, concat_axis=0, tiled=True)
    piece = jnp.sum(pieces.reshape(dom_count, -1, width).astype(F32), axis=0) * scale
    whole = lax.all_gather(piece.astype(BF), "dom", axis=0, tiled=True).astype(F32)
    cut = basis_count * quarter

    scaled_high = scaled.astype(BF)
    scaled_low = (scaled - scaled_high.astype(F32)).astype(BF)
    grad_coef = dot(relation_hot, scaled_high, 1, 1) + dot(relation_hot, scaled_low, 1, 1)
    coef_total = lax.psum(grad_coef, ("dom", "feat"))
    return (
        output,
        grad_feats,
        whole[:cut].reshape(basis_count, quarter, width),
        whole[cut:].T,
        coef_total * scale,
    )


def solution(mesh):
    return jax.shard_map(
        body,
        mesh=mesh,
        in_specs=(
            P("feat", "dom"),
            P(None, "feat"),
            P(None, "feat", None),
            P(),
            P("dom", None),
            P("dom"),
            P("dom"),
            P("dom"),
            P("dom", None),
            P("dom", None),
            P("feat", "dom"),
        ),
        out_specs=(P("feat", "dom"), P("feat", "dom"), P(None, "feat", None), P(None, "feat"), P()),
        check_vma=False,
    )
```

```python
import functools

import jax
import jax.numpy as jnp
from jax import lax
from jax.experimental import pallas as pl
from jax.experimental.pallas import tpu as pltpu
from jax.sharding import PartitionSpec as P

BF = jnp.bfloat16
F32 = jnp.float32


def dot(left, right, left_axis, right_axis):
    return lax.dot_general(
        left, right, (((left_axis,), (right_axis,)), ((), ())), preferred_element_type=F32
    )


def onehot(ids, start, size):
    return (jnp.arange(size, dtype=jnp.int32)[:, None] + start == ids[None, :]).astype(BF)


def pick(table, ids, chunk):
    width = table.shape[1]
    if width <= chunk:
        return dot(table, onehot(ids, 0, width), 1, 0).astype(BF)

    def step(index, total):
        piece = lax.dynamic_slice_in_dim(table, index * chunk, chunk, 1)
        return total + dot(piece, onehot(ids, index * chunk, chunk), 1, 0)

    total = lax.fori_loop(
        0, width // chunk, step, jnp.zeros((table.shape[0], ids.shape[0]), F32)
    )
    return total.astype(BF)


def spread(values, ids, width, chunk):
    if width <= chunk:
        return dot(values, onehot(ids, 0, width), 1, 1)

    def step(index, total):
        piece = dot(values, onehot(ids, index * chunk, chunk), 1, 1)
        return lax.dynamic_update_slice_in_dim(total, piece, index * chunk, 1)

    return lax.fori_loop(0, width // chunk, step, jnp.zeros((values.shape[0], width), F32))


def peers(axis, count):
    me = lax.axis_index(axis)
    return me, me // 2, me % 2, count // 2


def greet(axis, me, spot, side, columns):
    barrier = pltpu.get_barrier_semaphore()
    pl.semaphore_signal(
        barrier, inc=1, device_id={axis: spot * 2 + 1 - side}, device_id_type=pl.DeviceIdType.MESH
    )
    for hop in range(1, columns):
        other = (spot + hop) % columns
        pl.semaphore_signal(
            barrier, inc=1, device_id={axis: other * 2 + side}, device_id_type=pl.DeviceIdType.MESH
        )
    pl.semaphore_wait(barrier, columns)


def gather_kernel(axis, count, x_ref, o_ref, own_sem, send, recv, pair_send, pair_recv):
    me, spot, side, columns = peers(axis, count)
    mate = spot * 2 + 1 - side
    greet(axis, me, spot, side, columns)

    def remote(source, place, send_sem, recv_sem, target):
        return pltpu.make_async_remote_copy(
            src_ref=source,
            dst_ref=o_ref.at[place],
            send_sem=send_sem,
            recv_sem=recv_sem,
            device_id={axis: target},
            device_id_type=pl.DeviceIdType.MESH,
        )

    started = []
    for hop in range(1, columns):
        target = (spot + hop) % columns * 2 + side
        copy = remote(x_ref, me, send.at[hop - 1], recv.at[hop - 1], target)
        copy.start()
        started.append(copy)
    first = remote(x_ref, me, pair_send.at[0], pair_recv.at[0], mate)
    first.start()
    own = pltpu.make_async_copy(x_ref, o_ref.at[me], own_sem)
    own.start()
    passed = [first]
    for hop in range(1, columns):
        started[hop - 1].wait_recv()
        place = (spot - hop + columns) % columns * 2 + side
        copy = remote(o_ref.at[place], place, pair_send.at[hop], pair_recv.at[hop], mate)
        copy.start()
        passed.append(copy)
    own.wait()
    for copy in started:
        copy.wait_send()
    for copy in passed:
        copy.wait()


def all_gather(values, axis, count, ident):
    columns = count // 2
    return pl.pallas_call(
        functools.partial(gather_kernel, axis, count),
        out_shape=jax.ShapeDtypeStruct((count,) + values.shape, values.dtype),
        in_specs=[pl.BlockSpec(memory_space=pltpu.VMEM)],
        out_specs=pl.BlockSpec(memory_space=pltpu.VMEM),
        scratch_shapes=[
            pltpu.SemaphoreType.DMA,
            pltpu.SemaphoreType.DMA((columns - 1,)),
            pltpu.SemaphoreType.DMA((columns - 1,)),
            pltpu.SemaphoreType.DMA((columns,)),
            pltpu.SemaphoreType.DMA((columns,)),
        ],
        compiler_params=pltpu.CompilerParams(collective_id=ident, has_side_effects=True),
    )(values)


def reduce_kernel(
    axis, count, x_ref, o_ref, landed, summed, arrived, send, recv, pair_send, pair_recv
):
    me, spot, side, columns = peers(axis, count)
    mate = spot * 2 + 1 - side
    greet(axis, me, spot, side, columns)
    order = [(spot + hop) % columns for hop in list(range(1, columns)) + [0]]
    passed = []
    for step, place in enumerate(order):
        copy = pltpu.make_async_remote_copy(
            src_ref=x_ref.at[place * 2 + 1 - side],
            dst_ref=landed.at[step],
            send_sem=pair_send.at[step],
            recv_sem=pair_recv.at[step],
            device_id={axis: mate},
            device_id_type=pl.DeviceIdType.MESH,
        )
        copy.start()
        passed.append(copy)
    started = []
    for step, place in enumerate(order):
        passed[step].wait_recv()
        total = x_ref[place * 2 + side].astype(F32) + landed[step].astype(F32)
        summed[step] = total.astype(BF)
        if step < columns - 1:
            copy = pltpu.make_async_remote_copy(
                src_ref=summed.at[step],
                dst_ref=arrived.at[step],
                send_sem=send.at[step],
                recv_sem=recv.at[step],
                device_id={axis: place * 2 + side},
                device_id_type=pl.DeviceIdType.MESH,
            )
            copy.start()
            started.append(copy)
    total = summed[columns - 1].astype(F32)
    for step, copy in enumerate(started):
        copy.wait_recv()
        total = total + arrived[step].astype(F32)
    o_ref[...] = total
    for copy in started + passed:
        copy.wait_send()


def reduce_parts(values, axis, count, ident):
    columns = count // 2
    shape = values.shape[1:]
    return pl.pallas_call(
        functools.partial(reduce_kernel, axis, count),
        out_shape=jax.ShapeDtypeStruct(shape, F32),
        in_specs=[pl.BlockSpec(memory_space=pltpu.VMEM)],
        out_specs=pl.BlockSpec(memory_space=pltpu.VMEM),
        scratch_shapes=[
            pltpu.VMEM((columns,) + shape, BF),
            pltpu.VMEM((columns,) + shape, BF),
            pltpu.VMEM((columns - 1,) + shape, BF),
            pltpu.SemaphoreType.DMA((columns - 1,)),
            pltpu.SemaphoreType.DMA((columns - 1,)),
            pltpu.SemaphoreType.DMA((columns,)),
            pltpu.SemaphoreType.DMA((columns,)),
        ],
        compiler_params=pltpu.CompilerParams(collective_id=ident, has_side_effects=True),
    )(values)


def by_part(values, count):
    rows, columns = values.shape
    return values.reshape(rows, count, columns // count).transpose(1, 0, 2)


def side_by_side(parts):
    count, rows, columns = parts.shape
    return parts.transpose(1, 0, 2).reshape(rows, count * columns)


def group_of(count):
    return max(size for size in range(1, 6) if count % size == 0)


def forward_kernel(group, bases_ref, sources_ref, weights_ref, out_ref):
    basis_count, quarter, width = bases_ref.shape
    sources = sources_ref[...]

    def step(index, total):
        part = bases_ref[pl.ds(index * group, group)].reshape(group * quarter, width)
        products = jnp.dot(part, sources, preferred_element_type=F32)
        for k in range(group):
            weight = weights_ref[pl.ds(index * group + k, 1), :]
            total = total + products[k * quarter:(k + 1) * quarter] * weight
        return total

    total = lax.fori_loop(0, basis_count // group, step, jnp.zeros(out_ref.shape, F32))
    out_ref[...] = total.astype(BF)


def backward_kernel(
    group, bases_ref, sources_ref, weights_ref, grad_ref, bases_out, scaled_out, edge_out
):
    basis_count, quarter, width = bases_ref.shape
    sources = sources_ref[...]
    edge_out[...] = jnp.zeros(edge_out.shape, F32)

    def step(index, carry):
        part = bases_ref[pl.ds(index * group, group)].reshape(group * quarter, width)
        products = jnp.dot(part, sources, preferred_element_type=F32)
        grad = grad_ref[...].astype(F32)
        combined = []
        for k in range(group):
            spot = pl.ds(index * group + k, 1)
            scaled_out[spot, :] = jnp.sum(
                products[k * quarter:(k + 1) * quarter] * grad, axis=0, keepdims=True
            )
            combined.append((grad * weights_ref[spot, :]).astype(BF))
        combined = jnp.concatenate(combined, axis=0)
        piece = dot(combined, sources, 1, 1)
        bases_out[pl.ds(index * group, group)] = piece.reshape(group, quarter, width).astype(BF)
        edge_out[...] += dot(part, combined, 0, 0)
        return carry

    lax.fori_loop(0, basis_count // group, step, 0)


def body(
    feats,
    self_weight,
    bases,
    coef,
    src_part,
    src_row,
    edge_dst,
    edge_rel,
    block_owner,
    block_valid,
    cotangent,
):
    dom_count = lax.axis_size("dom")
    feat_count = lax.axis_size("feat")
    quarter, entities = feats.shape
    edge_count = src_row.shape[0]
    block_count = block_valid.shape[1]
    block_rows = edge_count // block_count
    basis_count, _, width = bases.shape
    relations = coef.shape[0]
    total_entities = dom_count * entities
    chunk = min(8, dom_count) * entities
    scale = float(edge_count * dom_count) ** (-0.5)

    source_ids = src_part[:, 0] * entities + src_row
    live = (jnp.arange(block_rows)[None, :] < block_valid[0][:, None]).reshape(edge_count)
    owners = jnp.broadcast_to(block_owner, (block_count, block_rows)).reshape(edge_count)
    target_ids = jnp.where(live, owners * entities + edge_dst, -1)
    relation_hot = onehot(edge_rel, 0, relations)

    table = side_by_side(all_gather(feats, "dom", dom_count, 0))
    source_quarter = pick(table, source_ids, chunk)
    gathered = all_gather(
        jnp.concatenate([source_quarter, feats], axis=1), "feat", feat_count, 1
    ).reshape(width, edge_count + entities)
    sources = gathered[:, :edge_count]
    own_full = gathered[:, edge_count:]

    group = group_of(basis_count)
    vmem = pl.BlockSpec(memory_space=pltpu.VMEM)
    first = coef.astype(BF)
    second = (coef - first.astype(F32)).astype(BF)
    third = (coef - first.astype(F32) - second.astype(F32)).astype(BF)
    weights = (
        dot(first, relation_hot, 0, 0)
        + dot(second, relation_hot, 0, 0)
        + dot(third, relation_hot, 0, 0)
    )
    messages = pl.pallas_call(
        functools.partial(forward_kernel, group),
        out_shape=jax.ShapeDtypeStruct((quarter, edge_count), BF),
        in_specs=[vmem] * 3,
        out_specs=vmem,
    )(bases, sources, weights)
    extra = 16
    tail = jnp.zeros((extra, edge_count), BF).at[0].set(1.0)
    partial = spread(jnp.concatenate([messages, tail], axis=0), target_ids, total_entities, chunk)
    counted = partial[quarter:quarter + 1]
    high = jnp.floor(counted / 64.0)
    counts = jnp.concatenate(
        [high, counted - 64.0 * high, jnp.zeros((extra - 2, total_entities), F32)], axis=0
    )
    sent = jnp.concatenate([partial[:quarter], counts], axis=0).astype(BF)
    arrived = reduce_parts(by_part(sent, dom_count), "dom", dom_count, 2)
    aggregate = arrived[:quarter]
    degree = arrived[quarter:quarter + 1] * 64.0 + arrived[quarter + 1:quarter + 2]
    inverse_degree = 1.0 / jnp.maximum(degree, 1.0)
    preact = dot(self_weight, own_full, 0, 0) + inverse_degree * aggregate
    output = jax.nn.silu(preact).astype(BF)
    sigmoid_pre = jax.nn.sigmoid(preact)
    grad_pre = (
        cotangent.astype(F32) * sigmoid_pre * (1.0 + preact * (1.0 - sigmoid_pre))
    ).astype(BF)
    grad_node = (grad_pre.astype(F32) * inverse_degree).astype(BF)
    grad_table = side_by_side(all_gather(grad_node, "dom", dom_count, 3))
    grad_message = pick(grad_table, target_ids, chunk)

    grad_bases, scaled, edge_partial = pl.pallas_call(
        functools.partial(backward_kernel, group),
        out_shape=(
            jax.ShapeDtypeStruct((basis_count, quarter, width), BF),
            jax.ShapeDtypeStruct((basis_count, edge_count), F32),
            jax.ShapeDtypeStruct((width, edge_count), F32),
        ),
        in_specs=[vmem] * 4,
        out_specs=(vmem,) * 3,
    )(bases, sources, weights, grad_message)
    self_partial = dot(self_weight, grad_pre, 1, 0)
    self_term = dot(grad_pre, own_full, 1, 1)

    scaled_high = scaled.astype(BF)
    scaled_low = (scaled - scaled_high.astype(F32)).astype(BF)
    grad_coef = dot(scaled_high, relation_hot, 1, 1) + dot(scaled_low, relation_hot, 1, 1)
    lanes = -(-relations // 256) * 256
    coef_size = -(-basis_count // 32) * 32 * lanes
    coef_wide = coef_size // quarter
    padded = jnp.pad(
        grad_coef, ((0, coef_size // lanes - basis_count), (0, lanes - relations))
    ).reshape(quarter, coef_wide)
    both = jnp.concatenate([edge_partial, self_partial], axis=1).reshape(feat_count, quarter, -1)
    spare = jnp.broadcast_to(padded[None], (feat_count, quarter, coef_wide))
    both = jnp.concatenate([both, spare], axis=2).astype(BF)
    both = reduce_parts(both, "feat", feat_count, 4)
    edge_grads = both[:, :edge_count].astype(BF)
    self_grads = both[:, edge_count:edge_count + entities]
    coef_sum = both[:, edge_count + entities:].reshape(-1, width).astype(BF)
    node_grads = by_part(
        spread(edge_grads, source_ids, total_entities, chunk).astype(BF), dom_count
    )

    cut = basis_count * quarter
    rows = cut + quarter + coef_sum.shape[0]
    more = -rows % (16 * dom_count)
    stacked = jnp.concatenate(
        [
            grad_bases.reshape(cut, width),
            self_term.astype(BF),
            coef_sum,
            jnp.zeros((more, width), BF),
        ],
        axis=0,
    ).reshape(dom_count, -1, width)
    height = stacked.shape[1]
    reduced = reduce_parts(
        jnp.concatenate([stacked, node_grads.reshape(dom_count, -1, width)], axis=1),
        "dom",
        dom_count,
        5,
    )
    grad_feats = (self_grads + reduced[height:].reshape(quarter, entities)).astype(BF)
    piece = (reduced[:height] * scale).astype(BF)
    whole = all_gather(piece, "dom", dom_count, 6).reshape(-1, width).astype(F32)
    coef_total = whole[cut + quarter:cut + quarter + coef_sum.shape[0]]
    coef_total = coef_total.reshape(-1, lanes)[:basis_count, :relations].T
    return (
        output,
        grad_feats,
        whole[:cut].reshape(basis_count, quarter, width),
        whole[cut:cut + quarter].T,
        coef_total,
    )


def solution(mesh):
    return jax.shard_map(
        body,
        mesh=mesh,
        in_specs=(
            P("feat", "dom"),
            P(None, "feat"),
            P(None, "feat", None),
            P(),
            P("dom", None),
            P("dom"),
            P("dom"),
            P("dom"),
            P("dom", None),
            P("dom", None),
            P("feat", "dom"),
        ),
        out_specs=(P("feat", "dom"), P("feat", "dom"), P(None, "feat", None), P(None, "feat"), P()),
        check_vma=False,
    )
```

```python
import functools

import jax
import jax.numpy as jnp
from jax import lax
from jax.experimental import pallas as pl
from jax.experimental.pallas import tpu as pltpu
from jax.sharding import PartitionSpec as P

BF = jnp.bfloat16
F32 = jnp.float32


def dot(left, right, left_axis, right_axis):
    return lax.dot_general(
        left, right, (((left_axis,), (right_axis,)), ((), ())), preferred_element_type=F32
    )


def onehot(ids, start, size):
    return (jnp.arange(size, dtype=jnp.int32)[:, None] + start == ids[None, :]).astype(BF)


def spread(values, ids, width, chunk):
    if width <= chunk:
        return dot(values, onehot(ids, 0, width), 1, 1)

    def step(index, total):
        piece = dot(values, onehot(ids, index * chunk, chunk), 1, 1)
        return lax.dynamic_update_slice_in_dim(total, piece, index * chunk, 1)

    return lax.fori_loop(0, width // chunk, step, jnp.zeros((values.shape[0], width), F32))


def peers(axis, count):
    me = lax.axis_index(axis)
    return me, me // 2, me % 2, count // 2


def greet(groups):
    barrier = pltpu.get_barrier_semaphore()
    expected = 0
    for axis, count in groups:
        me, spot, side, columns = peers(axis, count)
        targets = [spot * 2 + 1 - side]
        targets += [(spot + hop) % columns * 2 + side for hop in range(1, columns)]
        for target in targets:
            pl.semaphore_signal(
                barrier, inc=1, device_id={axis: target}, device_id_type=pl.DeviceIdType.MESH
            )
        expected += columns
    pl.semaphore_wait(barrier, expected)


def remote(source, target_ref, send_sem, recv_sem, axis, target):
    return pltpu.make_async_remote_copy(
        src_ref=source,
        dst_ref=target_ref,
        send_sem=send_sem,
        recv_sem=recv_sem,
        device_id={axis: target},
        device_id_type=pl.DeviceIdType.MESH,
    )


class Gather:
    def __init__(self, axis, count, x_ref, o_ref, own_sem, send, recv, pair_send, pair_recv):
        self.me, self.spot, self.side, self.columns = peers(axis, count)
        self.axis, self.o_ref = axis, o_ref
        self.mate = self.spot * 2 + 1 - self.side
        self.pair_send, self.pair_recv = pair_send, pair_recv
        self.started, self.passed = [], []
        for hop in range(1, self.columns):
            target = (self.spot + hop) % self.columns * 2 + self.side
            copy = remote(
                x_ref, o_ref.at[self.me], send.at[hop - 1], recv.at[hop - 1], axis, target
            )
            copy.start()
            self.started.append(copy)
        first = remote(
            x_ref, o_ref.at[self.me], pair_send.at[0], pair_recv.at[0], axis, self.mate
        )
        first.start()
        self.passed.append(first)
        self.own = pltpu.make_async_copy(x_ref, o_ref.at[self.me], own_sem)
        self.own.start()

    def place(self, hop, side):
        return (self.spot - hop + self.columns) % self.columns * 2 + side

    def forward(self, hop):
        self.started[hop - 1].wait_recv()
        place = self.place(hop, self.side)
        copy = remote(
            self.o_ref.at[place],
            self.o_ref.at[place],
            self.pair_send.at[hop],
            self.pair_recv.at[hop],
            self.axis,
            self.mate,
        )
        copy.start()
        self.passed.append(copy)
        return place

    def from_mate(self, hop):
        self.passed[hop].wait_recv()
        return self.place(hop, 1 - self.side)

    def finish(self):
        for copy in self.started + self.passed:
            copy.wait_send()


def gather_scratch(count):
    columns = count // 2
    return [
        pltpu.SemaphoreType.DMA,
        pltpu.SemaphoreType.DMA((columns - 1,)),
        pltpu.SemaphoreType.DMA((columns - 1,)),
        pltpu.SemaphoreType.DMA((columns,)),
        pltpu.SemaphoreType.DMA((columns,)),
    ]


class Reduce:
    def __init__(
        self, axis, count, x_ref, landed, summed, arrived, send, recv, pair_send, pair_recv
    ):
        me, spot, side, columns = peers(axis, count)
        self.axis, self.side, self.columns, self.x_ref = axis, side, columns, x_ref
        self.landed, self.summed, self.arrived = landed, summed, arrived
        self.send, self.recv = send, recv
        self.order = [(spot + hop) % columns for hop in list(range(1, columns)) + [0]]
        self.passed, self.started = [], []
        for step, place in enumerate(self.order):
            copy = remote(
                x_ref.at[place * 2 + 1 - side],
                landed.at[step],
                pair_send.at[step],
                pair_recv.at[step],
                axis,
                spot * 2 + 1 - side,
            )
            copy.start()
            self.passed.append(copy)

    def middle(self, step):
        place = self.order[step]
        self.passed[step].wait_recv()
        total = self.x_ref[place * 2 + self.side].astype(F32) + self.landed[step].astype(F32)
        self.summed[step] = total.astype(BF)
        if step < self.columns - 1:
            copy = remote(
                self.summed.at[step],
                self.arrived.at[step],
                self.send.at[step],
                self.recv.at[step],
                self.axis,
                place * 2 + self.side,
            )
            copy.start()
            self.started.append(copy)

    def finish(self, o_ref):
        total = self.summed[self.columns - 1].astype(F32)
        for step, copy in enumerate(self.started):
            copy.wait_recv()
            total = total + self.arrived[step].astype(F32)
        o_ref[...] = total
        for copy in self.started + self.passed:
            copy.wait_send()


def reduce_scratch(count, shape):
    columns = count // 2
    return [
        pltpu.VMEM((columns,) + shape, BF),
        pltpu.VMEM((columns,) + shape, BF),
        pltpu.VMEM((columns - 1,) + shape, BF),
        pltpu.SemaphoreType.DMA((columns - 1,)),
        pltpu.SemaphoreType.DMA((columns - 1,)),
        pltpu.SemaphoreType.DMA((columns,)),
        pltpu.SemaphoreType.DMA((columns,)),
    ]


def exchange(kernel, out_shape, args, scratch, ident):
    vmem = pl.BlockSpec(memory_space=pltpu.VMEM)
    return pl.pallas_call(
        kernel,
        out_shape=out_shape,
        in_specs=[vmem] * len(args),
        out_specs=jax.tree.map(lambda leaf: vmem, out_shape),
        scratch_shapes=scratch,
        compiler_params=pltpu.CompilerParams(collective_id=ident, has_side_effects=True),
    )(*args)


def all_gather(values, axis, count, ident):
    def kernel(x_ref, o_ref, *scratch):
        greet([(axis, count)])
        gather = Gather(axis, count, x_ref, o_ref, *scratch)
        for hop in range(1, gather.columns):
            gather.forward(hop)
        gather.own.wait()
        for hop in range(gather.columns):
            gather.from_mate(hop)
        gather.finish()

    shape = jax.ShapeDtypeStruct((count,) + values.shape, values.dtype)
    return exchange(kernel, shape, (values,), gather_scratch(count), ident)


def gather_pick(values, ids, axis, count, ident):
    def kernel(x_ref, ids_ref, o_ref, table, total, *scratch):
        extent = x_ref.shape[1]
        greet([(axis, count)])
        gather = Gather(axis, count, x_ref, table, *scratch)
        rows = lax.broadcasted_iota(jnp.int32, (extent, ids_ref.shape[1]), 0)

        def use(place):
            hot = jnp.where(rows + place * extent == ids_ref[...], 1.0, 0.0).astype(BF)
            total[...] += jnp.dot(table[place], hot, preferred_element_type=F32)

        total[...] = jnp.zeros(total.shape, F32)
        gather.own.wait()
        use(gather.me)
        for hop in range(1, gather.columns):
            use(gather.forward(hop))
        for hop in range(gather.columns):
            use(gather.from_mate(hop))
        o_ref[...] = total[...].astype(BF)
        gather.finish()

    shape = (values.shape[0], ids.shape[1])
    scratch = [pltpu.VMEM((count,) + values.shape, BF), pltpu.VMEM(shape, F32)]
    return exchange(
        kernel,
        jax.ShapeDtypeStruct(shape, BF),
        (values, ids),
        scratch + gather_scratch(count),
        ident,
    )


def reduce_parts(values, axis, count, ident):
    def kernel(x_ref, o_ref, *scratch):
        greet([(axis, count)])
        reduce = Reduce(axis, count, x_ref, *scratch)
        for step in range(reduce.columns):
            reduce.middle(step)
        reduce.finish(o_ref)

    shape = values.shape[1:]
    return exchange(
        kernel, jax.ShapeDtypeStruct(shape, F32), (values,), reduce_scratch(count, shape), ident
    )


def reduce_both(first, axis, count, second, other_axis, other_count, ident):
    def kernel(x_ref, y_ref, o_ref, p_ref, *scratch):
        greet([(axis, count), (other_axis, other_count)])
        short = Reduce(axis, count, x_ref, *scratch[:7])
        long = Reduce(other_axis, other_count, y_ref, *scratch[7:])
        for step in range(short.columns):
            short.middle(step)
        for step in range(long.columns):
            long.middle(step)
        short.finish(o_ref)
        long.finish(p_ref)

    shape, other = first.shape[1:], second.shape[1:]
    return exchange(
        kernel,
        (jax.ShapeDtypeStruct(shape, F32), jax.ShapeDtypeStruct(other, F32)),
        (first, second),
        reduce_scratch(count, shape) + reduce_scratch(other_count, other),
        ident,
    )


def reduce_gather(values, pieces, axis, count, ident):
    def kernel(x_ref, y_ref, o_ref, p_ref, *scratch):
        greet([(axis, count)])
        reduce = Reduce(axis, count, x_ref, *scratch[:7])
        gather = Gather(axis, count, y_ref, p_ref, *scratch[7:])
        for step in range(reduce.columns):
            reduce.middle(step)
        for hop in range(1, gather.columns):
            gather.forward(hop)
        gather.own.wait()
        reduce.finish(o_ref)
        for hop in range(gather.columns):
            gather.from_mate(hop)
        gather.finish()

    shape = values.shape[1:]
    return exchange(
        kernel,
        (
            jax.ShapeDtypeStruct(shape, F32),
            jax.ShapeDtypeStruct((count,) + pieces.shape, pieces.dtype),
        ),
        (values, pieces),
        reduce_scratch(count, shape) + gather_scratch(count),
        ident,
    )


def by_part(values, count):
    rows, columns = values.shape
    return values.reshape(rows, count, columns // count).transpose(1, 0, 2)


def group_of(count):
    return max(size for size in range(1, 6) if count % size == 0)


def forward_kernel(group, bases_ref, sources_ref, weights_ref, out_ref):
    basis_count, quarter, width = bases_ref.shape
    sources = sources_ref[...]

    def step(index, total):
        part = bases_ref[pl.ds(index * group, group)].reshape(group * quarter, width)
        products = jnp.dot(part, sources, preferred_element_type=F32)
        for k in range(group):
            weight = weights_ref[pl.ds(index * group + k, 1), :]
            total = total + products[k * quarter:(k + 1) * quarter] * weight
        return total

    total = lax.fori_loop(0, basis_count // group, step, jnp.zeros(out_ref.shape, F32))
    out_ref[...] = total.astype(BF)


def backward_kernel(
    group, bases_ref, sources_ref, weights_ref, grad_ref, bases_out, scaled_out, edge_out
):
    basis_count, quarter, width = bases_ref.shape
    sources = sources_ref[...]
    edge_out[...] = jnp.zeros(edge_out.shape, F32)

    def step(index, carry):
        part = bases_ref[pl.ds(index * group, group)].reshape(group * quarter, width)
        products = jnp.dot(part, sources, preferred_element_type=F32)
        grad = grad_ref[...].astype(F32)
        combined = []
        for k in range(group):
            spot = pl.ds(index * group + k, 1)
            scaled_out[spot, :] = jnp.sum(
                products[k * quarter:(k + 1) * quarter] * grad, axis=0, keepdims=True
            )
            combined.append((grad * weights_ref[spot, :]).astype(BF))
        combined = jnp.concatenate(combined, axis=0)
        piece = dot(combined, sources, 1, 1)
        bases_out[pl.ds(index * group, group)] = piece.reshape(group, quarter, width).astype(BF)
        edge_out[...] += dot(part, combined, 0, 0)
        return carry

    lax.fori_loop(0, basis_count // group, step, 0)


def body(
    feats,
    self_weight,
    bases,
    coef,
    src_part,
    src_row,
    edge_dst,
    edge_rel,
    block_owner,
    block_valid,
    cotangent,
):
    dom_count = lax.axis_size("dom")
    feat_count = lax.axis_size("feat")
    quarter, entities = feats.shape
    edge_count = src_row.shape[0]
    block_count = block_valid.shape[1]
    block_rows = edge_count // block_count
    basis_count, _, width = bases.shape
    relations = coef.shape[0]
    total_entities = dom_count * entities
    chunk = min(8, dom_count) * entities
    scale = float(edge_count * dom_count) ** (-0.5)

    source_ids = src_part[:, 0] * entities + src_row
    live = (jnp.arange(block_rows)[None, :] < block_valid[0][:, None]).reshape(edge_count)
    owners = jnp.broadcast_to(block_owner, (block_count, block_rows)).reshape(edge_count)
    target_ids = jnp.where(live, owners * entities + edge_dst, -1)
    relation_hot = onehot(edge_rel, 0, relations)

    source_quarter = gather_pick(feats, source_ids[None, :], "dom", dom_count, 0)
    gathered = all_gather(
        jnp.concatenate([source_quarter, feats], axis=1), "feat", feat_count, 1
    ).reshape(width, edge_count + entities)
    sources = gathered[:, :edge_count]
    own_full = gathered[:, edge_count:]

    group = group_of(basis_count)
    vmem = pl.BlockSpec(memory_space=pltpu.VMEM)
    first = coef.astype(BF)
    second = (coef - first.astype(F32)).astype(BF)
    third = (coef - first.astype(F32) - second.astype(F32)).astype(BF)
    weights = (
        dot(first, relation_hot, 0, 0)
        + dot(second, relation_hot, 0, 0)
        + dot(third, relation_hot, 0, 0)
    )
    messages = pl.pallas_call(
        functools.partial(forward_kernel, group),
        out_shape=jax.ShapeDtypeStruct((quarter, edge_count), BF),
        in_specs=[vmem] * 3,
        out_specs=vmem,
    )(bases, sources, weights)
    extra = 16
    tail = jnp.zeros((extra, edge_count), BF).at[0].set(1.0)
    partial = spread(jnp.concatenate([messages, tail], axis=0), target_ids, total_entities, chunk)
    counted = partial[quarter:quarter + 1]
    high = jnp.floor(counted / 64.0)
    counts = jnp.concatenate(
        [high, counted - 64.0 * high, jnp.zeros((extra - 2, total_entities), F32)], axis=0
    )
    sent = jnp.concatenate([partial[:quarter], counts], axis=0).astype(BF)
    arrived = reduce_parts(by_part(sent, dom_count), "dom", dom_count, 2)
    aggregate = arrived[:quarter]
    degree = arrived[quarter:quarter + 1] * 64.0 + arrived[quarter + 1:quarter + 2]
    inverse_degree = 1.0 / jnp.maximum(degree, 1.0)
    preact = dot(self_weight, own_full, 0, 0) + inverse_degree * aggregate
    output = jax.nn.silu(preact).astype(BF)
    sigmoid_pre = jax.nn.sigmoid(preact)
    grad_pre = (
        cotangent.astype(F32) * sigmoid_pre * (1.0 + preact * (1.0 - sigmoid_pre))
    ).astype(BF)
    grad_node = (grad_pre.astype(F32) * inverse_degree).astype(BF)
    grad_message = gather_pick(grad_node, target_ids[None, :], "dom", dom_count, 3)

    grad_bases, scaled, edge_partial = pl.pallas_call(
        functools.partial(backward_kernel, group),
        out_shape=(
            jax.ShapeDtypeStruct((basis_count, quarter, width), BF),
            jax.ShapeDtypeStruct((basis_count, edge_count), F32),
            jax.ShapeDtypeStruct((width, edge_count), F32),
        ),
        in_specs=[vmem] * 4,
        out_specs=(vmem,) * 3,
    )(bases, sources, weights, grad_message)
    self_partial = dot(self_weight, grad_pre, 1, 0)
    self_term = dot(grad_pre, own_full, 1, 1)

    scaled_high = scaled.astype(BF)
    scaled_low = (scaled - scaled_high.astype(F32)).astype(BF)
    grad_coef = dot(scaled_high, relation_hot, 1, 1) + dot(scaled_low, relation_hot, 1, 1)
    lanes = -(-relations // 256) * 256
    coef_size = -(-basis_count // 32) * 32 * lanes
    coef_wide = coef_size // quarter
    padded = jnp.pad(
        grad_coef, ((0, coef_size // lanes - basis_count), (0, lanes - relations))
    ).reshape(quarter, coef_wide)
    both = jnp.concatenate([edge_partial, self_partial], axis=1).reshape(feat_count, quarter, -1)
    spare = jnp.broadcast_to(padded[None], (feat_count, quarter, coef_wide))
    both = jnp.concatenate([both, spare], axis=2).astype(BF)
    cut = basis_count * quarter
    more = -(cut + quarter) % (16 * dom_count)
    stacked = jnp.concatenate(
        [grad_bases.reshape(cut, width), self_term.astype(BF), jnp.zeros((more, width), BF)],
        axis=0,
    ).reshape(dom_count, -1, width)
    both, piece = reduce_both(both, "feat", feat_count, stacked, "dom", dom_count, 4)
    edge_grads = both[:, :edge_count].astype(BF)
    self_grads = both[:, edge_count:edge_count + entities]
    coef_sum = both[:, edge_count + entities:].reshape(-1, width)
    node_grads = by_part(
        spread(edge_grads, source_ids, total_entities, chunk).astype(BF), dom_count
    )
    height = piece.shape[0]
    pieces = (jnp.concatenate([piece, coef_sum], axis=0) * scale).astype(BF)
    node_sum, gathered = reduce_gather(node_grads, pieces, "dom", dom_count, 5)
    grad_feats = (self_grads + node_sum).astype(BF)
    whole = gathered[:, :height].reshape(-1, width).astype(F32)
    coef_total = jnp.sum(gathered[:, height:].astype(F32), axis=0)
    coef_total = coef_total.reshape(-1, lanes)[:basis_count, :relations].T
    return (
        output,
        grad_feats,
        whole[:cut].reshape(basis_count, quarter, width),
        whole[cut:cut + quarter].T,
        coef_total,
    )


def solution(mesh):
    return jax.shard_map(
        body,
        mesh=mesh,
        in_specs=(
            P("feat", "dom"),
            P(None, "feat"),
            P(None, "feat", None),
            P(),
            P("dom", None),
            P("dom"),
            P("dom"),
            P("dom"),
            P("dom", None),
            P("dom", None),
            P("feat", "dom"),
        ),
        out_specs=(P("feat", "dom"), P("feat", "dom"), P(None, "feat", None), P(None, "feat"), P()),
        check_vma=False,
    )
```
